256 devices in a mesh: aa: 16 (over x, z_lo), ba: 16 (over z_hi, y, core).
Axes of the slice: x: 4, y: 4, z: 8 (z_hi: 2, z_lo: 4; z = z_hi * 4 + z_lo), core: 2. Of those that a mesh axis runs over, the one named last changes fastest.
Arguments:
- tokens: bfloat16 [16, 64, 256, 256], P('aa', 'ba'), may hold values from -6 to 6
- gain_attn: float32 [256], replicated, may hold values from 0.5 to 1.5
- fine_qkv: bfloat16 [256, 768], replicated, may hold values from -0.375 to 0.375
- fine_scale: float32 [4], replicated, may hold values from 8 to 32
- fine_out: bfloat16 [256, 256], replicated, may hold values from -0.375 to 0.375
- gain_mlp: float32 [256], replicated, may hold values from 0.5 to 1.5
- mlp_in: bfloat16 [256, 1536], replicated, may hold values from -0.375 to 0.375
- mlp_out: bfloat16 [768, 256], replicated, may hold values from -0.21875 to 0.21875
- merge_one: bfloat16 [1024, 512], P('aa'), may hold values from -0.1875 to 0.1875
- merge_two: bfloat16 [2048, 1024], P('aa'), may hold values from -0.125 to 0.125
- coarse_gain: float32 [1024], replicated, may hold values from 0.5 to 1.5
- coarse_qkv: bfloat16 [1024, 3072], P('aa'), may hold values from -0.1875 to 0.1875
- time_scale: float32 [16], replicated, may hold values from 8 to 32
- space_scale: float32 [16], replicated, may hold values from 8 to 32
- coarse_out: bfloat16 [2048, 1024], P('aa'), may hold values from -0.375 to 0.375
- split_two: bfloat16 [1024, 2048], P('aa'), may hold values from -0.1875 to 0.1875
- lerp_two: float32 [512], replicated, may hold values from 0.25 to 0.75
- split_one: bfloat16 [512, 1024], P('aa'), may hold values from -0.25 to 0.25
- lerp_one: float32 [256], replicated, may hold values from 0.25 to 0.75
Outputs:
- refined: bfloat16 [16, 64, 256, 256], P('aa', 'ba')
The draws below stay inside these ranges and needn't reach their ends.
All inputs are finite; a program needn't handle non-finite values.
Results may differ from the reference program's by a relative error of at most 0.014.
Values may be sent and summed in bfloat16 or wider, within the bound.
No kernel may reach another device: no remote copies, remote signals or barrier semaphores. Data moves between devices by JAX's collectives and lax.ppermute only.
A program may use at most 128 MiB of HBM per device.

```python
import math
import jax
import jax.numpy as jnp
from jax import lax

C = 256
C1 = 512
C2 = 1024
FFN = 768
W = 256
FRAMES = 16
H = 64
FINE_HEADS = 4
HEADS = 16


def shard_levels(own_key, shape, pieces, low, high):
    factor_of, own = 1.0, jax.random.fold_in(own_key, 6)
    for position, parts in pieces:
        steps = jnp.exp(jax.random.uniform(jax.random.fold_in(own, position), (parts,), jnp.float32, low / len(pieces), high / len(pieces)))
        factor_of = factor_of * jnp.repeat(steps, shape[position] // parts).reshape([-1 if axis == position else 1 for axis in range(len(shape))])
    return factor_of


def bell_draw(rng, extent, spread, most, shards=(), dtype=jnp.bfloat16):
    factor_of = shard_levels(rng, extent, shards, -0.22, 0.18) if shards else 1.0
    result = jax.random.normal(rng, extent, jnp.float32) * spread * factor_of
    return jnp.minimum(jnp.maximum(result, -most), most).astype(dtype)


def setup_inputs(seed: int = 0) -> dict:
    streams_of = jax.random.split(jax.random.key(seed), 20)
    tokens = bell_draw(streams_of[0], (FRAMES, H, W, C), 1.0, 6.0, ((0, 16), (1, 16)))
    gain_attn = jnp.clip(1.0 + 0.1 * jax.random.normal(streams_of[1], (C,), jnp.float32), 0.5, 1.5)
    fine_qkv = bell_draw(streams_of[2], (C, 3 * C), C ** -0.5, 0.375)
    fine_scale = jnp.clip(jnp.exp(jax.random.uniform(streams_of[3], (FINE_HEADS,), jnp.float32, math.log(8.0), math.log(32.0))), 8.0, 32.0)
    fine_out = bell_draw(streams_of[4], (C, C), C ** -0.5, 0.375)
    gain_mlp = jnp.clip(1.0 + 0.1 * jax.random.normal(streams_of[5], (C,), jnp.float32), 0.5, 1.5)
    mlp_in = bell_draw(streams_of[6], (C, 2 * FFN), C ** -0.5, 0.375)
    mlp_out = bell_draw(streams_of[7], (FFN, C), FFN ** -0.5, 0.21875)
    merge_one = bell_draw(streams_of[8], (4 * C, C1), (4 * C) ** -0.5, 0.1875, ((0, 16),))
    merge_two = bell_draw(streams_of[9], (4 * C1, C2), (4 * C1) ** -0.5, 0.125, ((0, 16),))
    coarse_gain = jnp.clip(1.0 + 0.1 * jax.random.normal(streams_of[10], (C2,), jnp.float32), 0.5, 1.5)
    coarse_qkv = bell_draw(streams_of[11], (C2, 3 * C2), C2 ** -0.5, 0.1875, ((0, 16),))
    time_scale = jnp.clip(jnp.exp(jax.random.uniform(streams_of[12], (HEADS,), jnp.float32, math.log(8.0), math.log(32.0))), 8.0, 32.0)
    space_scale = jnp.clip(jnp.exp(jax.random.uniform(streams_of[13], (HEADS,), jnp.float32, math.log(8.0), math.log(32.0))), 8.0, 32.0)
    coarse_out = bell_draw(streams_of[14], (2 * C2, C2), (2 * C2 // 9) ** -0.5, 0.375, ((0, 16),))
    split_two = bell_draw(streams_of[15], (C2, 4 * C1), C2 ** -0.5, 0.1875, ((0, 16),))
    lerp_two = jnp.clip(jax.random.uniform(streams_of[16], (C1,), jnp.float32, 0.25, 0.75), 0.25, 0.75)
    split_one = bell_draw(streams_of[17], (C1, 4 * C), C1 ** -0.5, 0.25, ((0, 16),))
    lerp_one = jnp.clip(jax.random.uniform(streams_of[18], (C,), jnp.float32, 0.25, 0.75), 0.25, 0.75)
    return {"tokens": tokens, "gain_attn": gain_attn, "fine_qkv": fine_qkv, "fine_scale": fine_scale, "fine_out": fine_out, "gain_mlp": gain_mlp, "mlp_in": mlp_in, "mlp_out": mlp_out, "merge_one": merge_one, "merge_two": merge_two, "coarse_gain": coarse_gain, "coarse_qkv": coarse_qkv, "time_scale": time_scale, "space_scale": space_scale, "coarse_out": coarse_out, "split_two": split_two, "lerp_two": lerp_two, "split_one": split_one, "lerp_one": lerp_one}


EPS = 1e-06

def rms_scale(value, gain):
    return value * lax.rsqrt(lax.optimization_barrier(jnp.mean(value * value, axis=-1, keepdims=True)) + EPS) * gain

def unit_axis(value, axis):
    return value * lax.rsqrt(lax.optimization_barrier(jnp.mean(value * value, axis=axis, keepdims=True)) + EPS)

def to_grid(part, head_size):
    row_count, col_count, width = part.shape
    return part.reshape(row_count, col_count, width // head_size, head_size).transpose(2, 3, 0, 1)

def window_attention(queries, key_grid, value_grid, row_ok, col_ok, scales):
    head_count, head_size, row_count, col_count = queries.shape
    factor = (scales / head_size)[:, None, None]
    query_wide = queries.astype(jnp.float32)
    weights = []
    for shift_row in range(7):
        for shift_col in range(7):
            key_part = key_grid[:, :, shift_row:shift_row + row_count, shift_col:shift_col + col_count].astype(jnp.float32)
            scores = lax.optimization_barrier(jnp.sum(query_wide * key_part, axis=1)) * factor
            usable = row_ok[shift_row:shift_row + row_count, None] * col_ok[None, shift_col:shift_col + col_count]
            weights.append(jnp.exp(scores) * usable)
    weight_sum = lax.optimization_barrier(jnp.sum(jnp.stack(weights), axis=0))
    numerator = jnp.zeros(queries.shape, jnp.float32)
    for shift_row in range(7):
        for shift_col in range(7):
            value_part = value_grid[:, :, shift_row:shift_row + row_count, shift_col:shift_col + col_count].astype(jnp.float32)
            numerator = numerator + weights[shift_row * 7 + shift_col][:, None] * value_part
    return numerator / weight_sum[:, None]

def finish_fine(stream, attended, fine_out, gain_mlp, mlp_in, mlp_out):
    row_count, col_count, width = stream.shape
    attended = attended.transpose(2, 3, 0, 1).reshape(row_count * col_count, width).astype(jnp.bfloat16)
    stream = stream + jnp.dot(attended, fine_out, preferred_element_type=jnp.float32).reshape(row_count, col_count, width)
    normed = rms_scale(stream, gain_mlp).astype(jnp.bfloat16)
    lifted = jnp.dot(normed.reshape(-1, width), mlp_in, preferred_element_type=jnp.float32)
    hidden_count = mlp_out.shape[0]
    hidden = (jax.nn.gelu(lifted[:, :hidden_count]) * lifted[:, hidden_count:]).astype(jnp.bfloat16)
    stream = stream + jnp.dot(hidden, mlp_out, preferred_element_type=jnp.float32).reshape(row_count, col_count, width)
    return stream.astype(jnp.bfloat16)

def fine_frame(one_frame, gain_attn, fine_qkv, fine_scale, fine_out, gain_mlp, mlp_in, mlp_out):
    row_count, col_count, width = one_frame.shape
    head_size = width // fine_scale.shape[0]
    stream = one_frame.astype(jnp.float32)
    normed = rms_scale(stream, gain_attn).astype(jnp.bfloat16)
    packed = jnp.dot(normed.reshape(-1, width), fine_qkv, preferred_element_type=jnp.float32).astype(jnp.bfloat16)
    packed = packed.reshape(row_count, col_count, 3 * width)
    queries = lax.optimization_barrier(unit_axis(to_grid(packed[:, :, :width], head_size).astype(jnp.float32), 1).astype(jnp.bfloat16))
    key_grid = lax.optimization_barrier(unit_axis(to_grid(packed[:, :, width:2 * width], head_size).astype(jnp.float32), 1).astype(jnp.bfloat16))
    value_grid = to_grid(packed[:, :, 2 * width:], head_size)
    margin = ((0, 0), (0, 0), (3, 3), (3, 3))
    key_grid = jnp.pad(key_grid, margin)
    value_grid = jnp.pad(value_grid, margin)
    row_ok = jnp.pad(jnp.ones((row_count,), jnp.float32), 3)
    col_ok = jnp.pad(jnp.ones((col_count,), jnp.float32), 3)
    attended = window_attention(queries, key_grid, value_grid, row_ok, col_ok, fine_scale)
    return finish_fine(stream, attended, fine_out, gain_mlp, mlp_in, mlp_out)

def patch_merge(grid):
    frame_count, row_count, col_count, width = grid.shape
    moved = grid.reshape(frame_count, row_count // 2, 2, col_count // 2, 2, width).transpose(0, 1, 3, 2, 4, 5)
    return moved.reshape(frame_count, row_count // 2, col_count // 2, 4 * width)

def patch_split(flat, frame_count, row_count, col_count):
    width = flat.shape[1] // 4
    moved = flat.reshape(frame_count, row_count, col_count, 2, 2, width).transpose(0, 1, 3, 2, 4, 5)
    return moved.reshape(frame_count, 2 * row_count, 2 * col_count, width)

def temporal(packed, scales):
    frame_count, place_count, total_width = packed.shape
    head_count = scales.shape[0]
    head_size = total_width // (3 * head_count)
    split_parts = packed.reshape(frame_count, place_count, head_count, 3, head_size)
    queries = lax.optimization_barrier(unit_axis(split_parts[:, :, :, 0].astype(jnp.float32), 3).astype(jnp.bfloat16))
    key_part = lax.optimization_barrier(unit_axis(split_parts[:, :, :, 1].astype(jnp.float32), 3).astype(jnp.bfloat16))
    value_part = split_parts[:, :, :, 2]
    scores = jnp.einsum('fphd,gphd->phfg', queries, key_part, preferred_element_type=jnp.float32)
    weights = jnp.exp(scores * (scales / head_size)[None, :, None, None])
    weight_sum = lax.optimization_barrier(jnp.sum(weights, axis=3))
    rounded = lax.optimization_barrier(weights.astype(jnp.bfloat16))
    merged = jnp.einsum('phfg,gphd->fphd', rounded, value_part, preferred_element_type=jnp.float32)
    merged = merged / weight_sum.transpose(2, 0, 1)[:, :, :, None]
    return merged.reshape(frame_count, place_count, head_count * head_size).astype(jnp.bfloat16)

def spatial(packed, scales):
    place_count, total_width = packed.shape
    head_count = scales.shape[0]
    head_size = total_width // (3 * head_count)
    split_parts = packed.reshape(place_count, head_count, 3, head_size)
    queries = lax.optimization_barrier(unit_axis(split_parts[:, :, 0].astype(jnp.float32), 2).astype(jnp.bfloat16)).transpose(1, 0, 2)
    key_part = lax.optimization_barrier(unit_axis(split_parts[:, :, 1].astype(jnp.float32), 2).astype(jnp.bfloat16)).transpose(1, 0, 2)
    value_part = split_parts[:, :, 2].transpose(1, 0, 2)
    block_rows = math.gcd(place_count, 512)
    factor = (scales / head_size)[:, None, None]
    blocks = queries.reshape(head_count, place_count // block_rows, block_rows, head_size).transpose(1, 0, 2, 3)

    def one_block(query_block):
        scores = jnp.einsum('hqd,hkd->hqk', query_block, key_part, preferred_element_type=jnp.float32) * factor
        weights = jnp.exp(scores)
        weight_sum = lax.optimization_barrier(jnp.sum(weights, axis=2))
        rounded = lax.optimization_barrier(weights.astype(jnp.bfloat16))
        merged = jnp.einsum('hqk,hkd->hqd', rounded, value_part, preferred_element_type=jnp.float32)
        return merged / weight_sum[:, :, None]
    results = lax.map(one_block, blocks)
    return results.transpose(0, 2, 1, 3).reshape(place_count, head_count * head_size).astype(jnp.bfloat16)

def reference(tokens, gain_attn, fine_qkv, fine_scale, fine_out, gain_mlp, mlp_in, mlp_out, merge_one, merge_two, coarse_gain, coarse_qkv, time_scale, space_scale, coarse_out, split_two, lerp_two, split_one, lerp_one):
    frame_count, row_count, col_count, width = tokens.shape

    def fine_one(one_frame):
        return fine_frame(one_frame, gain_attn, fine_qkv, fine_scale, fine_out, gain_mlp, mlp_in, mlp_out)
    level_zero = lax.map(fine_one, tokens)
    flat_one = patch_merge(level_zero).reshape(-1, 4 * width)
    level_one = jnp.dot(flat_one, merge_one, preferred_element_type=jnp.float32).astype(jnp.bfloat16)
    grid_one = level_one.reshape(frame_count, row_count // 2, col_count // 2, -1)
    flat_two = patch_merge(grid_one).reshape(-1, 4 * grid_one.shape[3])
    coarse = jnp.dot(flat_two, merge_two, preferred_element_type=jnp.float32)
    coarse_width = coarse.shape[1]
    place_count = row_count // 4 * (col_count // 4)
    normed = rms_scale(coarse, coarse_gain).astype(jnp.bfloat16)
    packed = jnp.dot(normed, coarse_qkv, preferred_element_type=jnp.float32).astype(jnp.bfloat16)
    packed = packed.reshape(frame_count, place_count, 3 * coarse_width)
    time_out = temporal(packed, time_scale)
    space_out = lax.map(lambda frame_packed: spatial(frame_packed, space_scale), packed)
    attended = jnp.concatenate([time_out, space_out], axis=2).reshape(-1, 2 * coarse_width)
    coarse = coarse + jnp.dot(attended, coarse_out, preferred_element_type=jnp.float32)
    raised = jnp.dot(coarse.astype(jnp.bfloat16), split_two, preferred_element_type=jnp.float32)
    raised_grid = patch_split(raised, frame_count, row_count // 4, col_count // 4)
    skip_one = grid_one.astype(jnp.float32)
    blended = (skip_one + lerp_two * (raised_grid - skip_one)).astype(jnp.bfloat16)
    raised = jnp.dot(blended.reshape(-1, blended.shape[3]), split_one, preferred_element_type=jnp.float32)
    raised_grid = patch_split(raised, frame_count, row_count // 2, col_count // 2)
    skip_zero = level_zero.astype(jnp.float32)
    return (skip_zero + lerp_one * (raised_grid - skip_zero)).astype(jnp.bfloat16)
```

```python
import jax
import jax.numpy as jnp
from jax import lax
from jax.experimental import pallas as pl
from jax.experimental.pallas import tpu as pltpu
from jax.sharding import Mesh
from jax.sharding import PartitionSpec as P

AA = ("x", "zl")
BA = ("zh", "yh", "yl", "c")
GROUP = ("yl", "c")
ACROSS = ("zh", "yh")
Y = ("yh", "yl")

EPS = 1e-06
HALO = 3
PAD = 16
TILE = 64
SPAN = TILE + 2 * PAD
HEAD = 64
FAR = -1e30
F32 = jnp.float32
BF16 = jnp.bfloat16
VMEM_LIMIT = 60 * 1024 * 1024


def dot(a, b):
    return jnp.dot(a, b, preferred_element_type=F32)


def dot_nt(a, b):
    return lax.dot_general(a, b, (((1,), (1,)), ((), ())), preferred_element_type=F32)


def rms_scale(value, gain):
    return value * lax.rsqrt(jnp.mean(value * value, axis=-1, keepdims=True) + EPS) * gain


def head_sums(width):
    row = lax.broadcasted_iota(jnp.int32, (width, width), 0) // HEAD
    col = lax.broadcasted_iota(jnp.int32, (width, width), 1) // HEAD
    return jnp.where(row == col, 1.0 / HEAD, 0.0).astype(BF16)


def unit_heads(value, sums):
    square = value * value
    high = square.astype(BF16)
    low = (square - high.astype(F32)).astype(BF16)
    return value * lax.rsqrt(dot(high, sums) + dot(low, sums) + EPS)


def call(body, out_shape, scratch=(), smem=0, count=0):
    specs = [pl.BlockSpec(memory_space=pltpu.SMEM)] * smem + [
        pl.BlockSpec(memory_space=pltpu.VMEM)
    ] * (count - smem)
    return pl.pallas_call(
        body,
        in_specs=specs,
        out_shape=out_shape,
        scratch_shapes=list(scratch),
        compiler_params=pltpu.CompilerParams(vmem_limit_bytes=VMEM_LIMIT),
    )


def fine_body(
    place_ref,
    scale_ref,
    own_ref,
    above_ref,
    below_ref,
    gain_ref,
    qkv_ref,
    out_w_ref,
    gain_mlp_ref,
    mlp_in_ref,
    mlp_out_ref,
    level_ref,
    flat_ref,
    q_s,
    k_s,
    v_s,
    mix_s,
    row_s,
):
    rows, cols, width = own_ref.shape
    heads = width // HEAD
    sums = head_sums(width)
    gain = gain_ref[...]
    edge = jnp.zeros((PAD, width), BF16)
    for r in range(rows + 2 * HALO):
        own = HALO <= r < HALO + rows
        if own:
            tile = own_ref[r - HALO]
        elif r < HALO:
            tile = above_ref[r]
        else:
            tile = below_ref[r - HALO - rows]
        normed = rms_scale(tile.astype(F32), gain).astype(BF16)
        if own:
            q = dot(normed, qkv_ref[:, :width]).astype(BF16)
            q_s[r - HALO] = unit_heads(q.astype(F32), sums).astype(BF16)
        k = dot(normed, qkv_ref[:, width : 2 * width]).astype(BF16)
        v = dot(normed, qkv_ref[:, 2 * width :]).astype(BF16)
        k_s[r, pl.ds(PAD, cols), :] = unit_heads(k.astype(F32), sums).astype(BF16)
        v_s[r, pl.ds(PAD, cols), :] = v
        k_s[r, pl.ds(0, PAD), :] = edge
        v_s[r, pl.ds(0, PAD), :] = edge
        k_s[r, pl.ds(PAD + cols, PAD), :] = edge
        v_s[r, pl.ds(PAD + cols, PAD), :] = edge

    reach = 2 * HALO + 1
    keys = reach * SPAN
    key_lane = lax.broadcasted_iota(jnp.int32, (TILE, keys), 1)
    shift = key_lane % SPAN - PAD - lax.broadcasted_iota(jnp.int32, (TILE, keys), 0)
    band = (shift >= -HALO) & (shift <= HALO)
    key_col = key_lane % SPAN - PAD
    key_row = key_lane // SPAN - HALO
    lane_head = lax.broadcasted_iota(jnp.int32, (TILE, width), 1) // HEAD
    total_rows = place_ref[1]
    tiles = cols // TILE

    def one_tile(step, carry):
        r = step // tiles
        start = pl.multiple_of((step % tiles) * TILE, TILE)
        q = q_s[r, pl.ds(start, TILE), :]
        none = jnp.zeros_like(q)
        stacked = jnp.concatenate(
            [jnp.where(lane_head == h, q, none) for h in range(heads)], axis=0
        )
        k = k_s[pl.ds(r, reach), pl.ds(start, SPAN), :].reshape(keys, width)
        v = v_s[pl.ds(r, reach), pl.ds(start, SPAN), :].reshape(keys, width)
        scores = dot_nt(stacked, k)
        row = key_row + (place_ref[0] + r)
        col = key_col + start
        ok = band & (row >= 0) & (row < total_rows) & (col >= 0) & (col < cols)
        bias = jnp.where(ok, 0.0, FAR)
        mixed = jnp.zeros((TILE, width), F32)
        weights = []
        totals = []
        for h in range(heads):
            part = scores[h * TILE : (h + 1) * TILE] * scale_ref[h] + bias
            weight = jnp.exp(part)
            totals.append(jnp.sum(weight, axis=1, keepdims=True))
            weights.append(weight.astype(BF16))
        summed = dot(jnp.concatenate(weights, axis=0), v)
        for h in range(heads):
            mixed = mixed + jnp.where(
                lane_head == h, summed[h * TILE : (h + 1) * TILE] / totals[h], 0.0
            )
        mix_s[r, pl.ds(start, TILE), :] = mixed.astype(BF16)
        return carry

    lax.fori_loop(0, rows * tiles, one_tile, 0)

    hidden_count = mlp_out_ref.shape[0]
    for r in range(rows):
        stream = own_ref[r].astype(F32) + dot(mix_s[r], out_w_ref[...])
        normed = rms_scale(stream, gain_mlp_ref[...]).astype(BF16)
        lifted = dot(normed, mlp_in_ref[...])
        hidden = (
            jax.nn.gelu(lifted[:, :hidden_count], approximate=True) * lifted[:, hidden_count:]
        ).astype(BF16)
        level = (stream + dot(hidden, mlp_out_ref[...])).astype(BF16)
        level_ref[r] = level
        row_s[...] = level.astype(F32).reshape(cols, width // 128, 128)
        for j in range(2):
            at = ((r % 2) * 2 + j) * width
            for g in range(width // 128):
                flat_ref[r // 2, :, pl.ds(at + g * 128, 128)] = row_s[
                    pl.ds(j, cols // 2, stride=2), g, :
                ].astype(BF16)


def merge_body(flat_ref, weight_ref, out_ref, row_s):
    rows, cols, _ = flat_ref.shape
    depth = weight_ref.shape[1]
    for i in range(rows):
        level = dot(flat_ref[i], weight_ref[...]).astype(BF16)
        row_s[...] = level.astype(F32).reshape(cols, depth // 128, 128)
        for j in range(2):
            at = (i * 2 + j) * depth
            for g in range(depth // 128):
                out_ref[:, pl.ds(at + g * 128, 128)] = row_s[
                    pl.ds(j, cols // 2, stride=2), g, :
                ].astype(BF16)


def coarse_body(low_ref, high_ref, pack_ref, out_ref):
    weight = pack_ref[:, :, :256].reshape(2048, 256)
    low = low_ref[...].reshape(256, 1024)
    high = high_ref[...].reshape(256, 1024)
    out_ref[...] = (dot(low, weight[:1024]) + dot(high, weight[1024:])).astype(BF16)


def qkv_body(parts_ref, gain_ref, pack_ref, time_ref, space_ref):
    value = jnp.concatenate([parts_ref[i] for i in range(4)], axis=1).astype(F32)
    normed = rms_scale(value, gain_ref[...]).astype(BF16)
    sums = head_sums(384)
    lane = lax.broadcasted_iota(jnp.int32, (256, 384), 1) // HEAD
    for h in range(2):
        weight = pack_ref[:, h * 64 : (h + 1) * 64, 256:640].reshape(1024, 384)
        packed = dot(normed, weight).astype(BF16)
        wide = packed.astype(F32)
        unit = jnp.where(lane % 3 == 2, wide, unit_heads(wide, sums)).astype(BF16)
        time_ref[:, pl.ds(h * 384, 384)] = unit
        space_ref[2 * h] = unit[:, :192]
        space_ref[2 * h + 1] = unit[:, 192:]


def time_body(scale_ref, packed_ref, out_ref):
    packed = packed_ref[...].reshape(256, 768)
    same = (
        lax.broadcasted_iota(jnp.int32, (256, 256), 0) % 16
        == lax.broadcasted_iota(jnp.int32, (256, 256), 1) % 16
    )
    bias = jnp.where(same, 0.0, FAR)
    results = []
    for h in range(4):
        part = packed[:, h * 192 : (h + 1) * 192]
        weight = jnp.exp(dot_nt(part[:, :64], part[:, 64:128]) * scale_ref[h] + bias)
        total = jnp.sum(weight, axis=1, keepdims=True)
        results.append(dot(weight.astype(BF16), part[:, 128:]) / total)
    out_ref[...] = jnp.concatenate(results, axis=1).astype(BF16).reshape(16, 16, 256)


def space_body(scale_ref, packed_ref, out_ref):
    k = packed_ref[:, :, 64:128].reshape(1024, 64)
    v = packed_ref[:, :, 128:192].reshape(1024, 64)
    for i in range(4):
        q = packed_ref[i, :, :64]
        weight = jnp.exp(dot_nt(q, k) * scale_ref[0])
        total = jnp.sum(weight, axis=1, keepdims=True)
        out_ref[i] = (dot(weight.astype(BF16), v) / total).astype(BF16)


def finish_body(
    core_ref,
    time_ref,
    space_ref,
    coarse_ref,
    mine_ref,
    other_ref,
    last_ref,
    one_ref,
    lerp_two_ref,
    level_ref,
    lerp_one_ref,
    out_ref,
    row_s,
):
    first = core_ref[0] == 0
    attended = [time_ref[g] for g in range(4)] + [space_ref[g] for g in range(4)]
    attended = jnp.concatenate(attended, axis=1)

    def halves(product):
        a = product(mine_ref)
        b = product(other_ref)
        return jnp.concatenate([jnp.where(first, a, b), jnp.where(first, b, a)], axis=1)

    def mixed(ref):
        return jnp.concatenate(
            [dot(attended, ref[y, :, :, :128].reshape(2048, 128)) for y in range(4)], axis=1
        )

    coarse = jnp.concatenate([coarse_ref[g] for g in range(4)], axis=1).astype(F32)
    coarse = (coarse + halves(mixed)).astype(BF16)

    def raised(ref):
        return jnp.concatenate(
            [
                dot(coarse, ref[y, :, h * 64 : (h + 1) * 64, 128:256].reshape(1024, 128))
                for y in range(4)
                for h in range(2)
            ],
            axis=1,
        )

    raised_two = halves(raised)
    skip = one_ref[...].astype(F32)
    lerp = jnp.concatenate([lerp_two_ref[...]] * 4, axis=1)
    blended = (skip + lerp * (raised_two - skip)).astype(BF16)
    stacked = jnp.concatenate([blended[:, p * 512 : (p + 1) * 512] for p in range(4)], axis=0)
    lerp_one = lerp_one_ref[...]
    weights = [
        last_ref[:, q * 32 : (q + 1) * 32, 256:512].reshape(512, 256) for q in range(4)
    ]
    cols = level_ref.shape[1]
    products = [dot(stacked, w) for w in weights]
    for i in range(2):
        for i2 in range(2):
            for j in range(2):
                for j2 in range(2):
                    p = i * 2 + j
                    tile = products[i2 * 2 + j2][p * 64 : (p + 1) * 64]
                    for g in range(2):
                        row_s[pl.ds(2 * j + j2, cols // 4, stride=4), g, :] = tile[
                            :, g * 128 : (g + 1) * 128
                        ]
            r = 2 * i + i2
            new = row_s[...].reshape(cols, 256)
            old = level_ref[r].astype(F32)
            out_ref[r] = (old + lerp_one * (new - old)).astype(BF16)


def sent_to_all(shard, axis):
    length = lax.axis_size(axis)
    return lax.all_to_all(
        jnp.broadcast_to(shard[None], (length, *shard.shape)), axis, 0, 0, tiled=True
    )


def rows_of(shard):
    for axis in ("zl", "x"):
        tiles = sent_to_all(shard, axis)
        shard = tiles.reshape(-1, shard.shape[1])
    return shard


def columns(shard, index, count):
    width = shard.shape[1] // count
    return lax.dynamic_slice_in_dim(shard, index * width, width, axis=1)


def stack_columns(shard, count):
    width = shard.shape[1] // count
    return jnp.concatenate([shard[:, i * width : (i + 1) * width] for i in range(count)], axis=0)


def shards(
    tokens,
    gain_attn,
    fine_qkv,
    fine_scale,
    fine_out,
    gain_mlp,
    mlp_in,
    mlp_out,
    merge_one,
    merge_two,
    coarse_gain,
    coarse_qkv,
    time_scale,
    space_scale,
    coarse_out,
    split_two,
    lerp_two,
    split_one,
    lerp_one,
):
    own = tokens[0]
    rows, cols, width = own.shape
    slab = lax.axis_index(BA)
    slabs = lax.axis_size(BA)
    above = lax.ppermute(own[rows - HALO :], BA, [(i, i + 1) for i in range(slabs - 1)])
    below = lax.ppermute(own[:HALO], BA, [(i + 1, i) for i in range(slabs - 1)])

    core = lax.axis_index("c")
    quarter = lax.axis_index(GROUP)
    part = core * 4 + lax.axis_index(Y)
    one_all = rows_of(merge_one)
    second = rows_of(
        jnp.concatenate(
            [columns(merge_two, quarter, 4), stack_columns(columns(coarse_qkv, quarter, 4), 2)],
            axis=1,
        )
    ).reshape(16, 128, 640)
    third = rows_of(
        jnp.concatenate(
            [
                columns(coarse_out, part, 8),
                stack_columns(columns(split_two, part, 8), 2),
                stack_columns(split_one, 4),
            ],
            axis=1,
        )
    )
    mine = sent_to_all(third[:, :256], Y).reshape(4, 16, 128, 256)
    other = lax.ppermute(mine, "c", [(0, 1), (1, 0)])
    third = third.reshape(16, 128, 512)

    place = jnp.stack([slab * rows, slabs * rows]).astype(jnp.int32)
    padded = cols + 2 * PAD
    level_zero, flat_one = call(
        fine_body,
        (
            jax.ShapeDtypeStruct((rows, cols, width), BF16),
            jax.ShapeDtypeStruct((rows // 2, cols // 2, 4 * width), BF16),
        ),
        [
            pltpu.VMEM((rows, cols, width), BF16),
            pltpu.VMEM((rows + 2 * HALO, padded, width), BF16),
            pltpu.VMEM((rows + 2 * HALO, padded, width), BF16),
            pltpu.VMEM((rows, cols, width), BF16),
            pltpu.VMEM((cols, width // 128, 128), F32),
        ],
        smem=2,
        count=11,
    )(
        place,
        fine_scale / HEAD,
        own,
        above,
        below,
        gain_attn[None],
        fine_qkv,
        fine_out,
        gain_mlp[None],
        mlp_in,
        mlp_out,
    )
    flat_two = call(
        merge_body,
        jax.ShapeDtypeStruct((cols // 4, 2048), BF16),
        [pltpu.VMEM((cols // 2, 4, 128), F32)],
        count=2,
    )(flat_one, one_all)
    low = lax.all_gather(flat_two[:, :1024], GROUP, axis=0)
    high = lax.all_gather(flat_two[:, 1024:], GROUP, axis=0)
    coarse_part = call(coarse_body, jax.ShapeDtypeStruct((256, 256), BF16), count=3)(
        low, high, second
    )
    coarse_parts = lax.all_gather(coarse_part, GROUP, axis=0)
    for_time, for_space = call(
        qkv_body,
        (jax.ShapeDtypeStruct((256, 768), BF16), jax.ShapeDtypeStruct((4, 256, 192), BF16)),
        count=3,
    )(coarse_parts, coarse_gain[None], second)
    time_in = lax.all_to_all(for_time.reshape(16, 16, 768), AA, 0, 0, tiled=True)
    space_in = lax.all_to_all(for_space, ACROSS, 0, 0, tiled=True)
    head = quarter * 4 + lax.axis_index(ACROSS)
    space_out = call(
        space_body, jax.ShapeDtypeStruct((4, 256, 64), BF16), smem=1, count=2
    )(lax.dynamic_slice_in_dim(space_scale / HEAD, head, 1), space_in)
    space_back = lax.all_to_all(space_out, ACROSS, 0, 0, tiled=True)
    time_out = call(time_body, jax.ShapeDtypeStruct((16, 16, 256), BF16), smem=1, count=2)(
        lax.dynamic_slice_in_dim(time_scale / HEAD, quarter * 4, 4), time_in
    )
    time_back = lax.all_to_all(time_out, AA, 0, 0, tiled=True)
    both = jnp.concatenate(
        [
            time_back.reshape(4, 64, 256),
            space_back.reshape(4, 4, 64, 64).transpose(1, 2, 0, 3).reshape(4, 64, 256),
        ],
        axis=2,
    )
    both = lax.all_to_all(both, GROUP, 0, 0, tiled=True)
    own_coarse = lax.dynamic_slice_in_dim(coarse_parts, quarter * 64, 64, axis=1)
    refined = call(
        finish_body,
        jax.ShapeDtypeStruct((rows, cols, width), BF16),
        [pltpu.VMEM((cols, 2, 128), F32)],
        smem=1,
        count=11,
    )(
        core.reshape(1).astype(jnp.int32),
        both[:, :, :256],
        both[:, :, 256:],
        own_coarse,
        mine,
        other,
        third,
        flat_two,
        lerp_two[None],
        level_zero,
        lerp_one[None],
    )
    return refined[None]


def solution(mesh):
    torus = Mesh(
        mesh.devices.reshape(4, 4, 2, 2, 2, 2), ("x", "zl", "zh", "yh", "yl", "c")
    )
    return jax.shard_map(
        shards,
        mesh=torus,
        in_specs=(
            P(AA, BA, None, None),
            P(),
            P(),
            P(),
            P(),
            P(),
            P(),
            P(),
            P(AA, None),
            P(AA, None),
            P(),
            P(AA, None),
            P(),
            P(),
            P(AA, None),
            P(AA, None),
            P(),
            P(AA, None),
            P(),
        ),
        out_specs=P(AA, BA, None, None),
        check_vma=False,
    )
```
